16 devices in a mesh: dp: 2 (over z), tp: 8 (over y, x, core).
Axes of the slice: x: 2, y: 2, z: 2, core: 2. Of those that a mesh axis runs over, the one named last changes fastest.
Arguments:
- out_y1: float32 [16, 1024, 1280], P('dp'), parts along dimension 0
- out_y2: float32 [16, 1024, 1280], P('dp'), parts along dimension 0
- cot_y1: float32 [16, 1024, 1280], P('dp'), parts along dimension 0
- cot_y2: float32 [16, 1024, 1280], P('dp'), parts along dimension 0
- w_qkv: bfloat16 [1, 1280, 16, 3, 80], P(None, None, 'tp')
- w_out: bfloat16 [1, 16, 80, 1280], P(None, 'tp')
- w_up: bfloat16 [1, 1280, 5120], P(None, None, 'tp')
- w_down: bfloat16 [1, 5120, 1280], P(None, 'tp')
Outputs:
- output 1: float32 [16, 1024, 1280], P('dp'), parts along dimension 0
- output 2: float32 [16, 1024, 1280], P('dp'), parts along dimension 0
- output 3: float32 [16, 1024, 1280], P('dp'), parts along dimension 0
- output 4: float32 [16, 1024, 1280], P('dp'), parts along dimension 0
- output 5: float32 [2, 1280, 16, 3, 80], P('dp', None, 'tp'), parts along dimension 0
- output 6: float32 [2, 16, 80, 1280], P('dp', 'tp'), parts along dimension 0
- output 7: float32 [2, 1280, 5120], P('dp', None, 'tp'), parts along dimension 0
- output 8: float32 [2, 5120, 1280], P('dp', 'tp'), parts along dimension 0
There are 2 independent parts. The reference program is written for one: setup_inputs(seed, part) draws one part's arguments, and reference() takes and returns one part's arrays. A program takes and returns all parts, laid end to end along the dimension named above; an argument that names none is the same for every part.
All inputs are finite; a program needn't handle non-finite values.
Results may differ from the reference program's by a relative error of at most 0.0124101.
Values are sent between devices in bfloat16 or wider.
A program may use at most 1.5 GiB of HBM per device.

```python
import math
import jax
import jax.numpy as jnp
from jax import lax

D = 1280
HEADS = 16
FF = 5120
SEQ = 1024
SEQS_DEV = 1
LAYERS = 1
TP = 8

BATCH = SEQS_DEV * TP
HEAD = D // HEADS
TOKENS = BATCH * SEQ
SCORE_SCALE = 1.0 / math.sqrt(HEAD)
NORM_EPS = 1e-6


def setup_inputs(seed: int = 0, part: int = 0) -> dict:
    weight_keys = jax.random.split(jax.random.key(seed), 4)
    act_keys = jax.random.split(jax.random.fold_in(jax.random.key(seed + 1), part), 4)
    act_shape = (BATCH, SEQ, D)
    in_scale = 1.0 / math.sqrt(D)
    hid_scale = 1.0 / math.sqrt(FF)
    attn_gain = max(1.0, math.sqrt(SEQ / 55.0))
    qkv_gain = jnp.array([1.4142, 1.4142, 1.0], jnp.float32).reshape(1, 1, 1, 3, 1)
    w_qkv = jax.random.normal(weight_keys[0], (LAYERS, D, HEADS, 3, HEAD), jnp.float32) * qkv_gain * in_scale
    w_out = jax.random.normal(weight_keys[1], (LAYERS, HEADS, HEAD, D), jnp.float32) * (0.4 * attn_gain * in_scale)
    w_up = jax.random.normal(weight_keys[2], (LAYERS, D, FF), jnp.float32) * in_scale
    w_down = jax.random.normal(weight_keys[3], (LAYERS, FF, D), jnp.float32) * (0.6 * hid_scale)
    return {
        "out_y1": jax.random.normal(act_keys[0], act_shape, jnp.float32),
        "out_y2": jax.random.normal(act_keys[1], act_shape, jnp.float32),
        "cot_y1": jax.random.normal(act_keys[2], act_shape, jnp.float32),
        "cot_y2": jax.random.normal(act_keys[3], act_shape, jnp.float32),
        "w_qkv": w_qkv.astype(jnp.bfloat16),
        "w_out": w_out.astype(jnp.bfloat16),
        "w_up": w_up.astype(jnp.bfloat16),
        "w_down": w_down.astype(jnp.bfloat16),
    }


def rms_fwd(x_in):
    inv_rms = lax.rsqrt(jnp.mean(x_in * x_in, axis=-1, keepdims=True) + NORM_EPS)
    return inv_rms, x_in * inv_rms


def rms_back(inv_rms, normed, grad_n):
    return inv_rms * (grad_n - normed * jnp.mean(normed * grad_n, axis=-1, keepdims=True))


def mlp_block(x_in, cot_out, w_up, w_down):
    inv_rms, normed = rms_fwd(x_in)
    n_bf = normed.astype(jnp.bfloat16)
    hidden = jnp.dot(n_bf, w_up, preferred_element_type=jnp.float32)
    act_f, gelu_back = jax.vjp(jax.nn.gelu, hidden)
    act_bf = act_f.astype(jnp.bfloat16)
    branch = jnp.dot(act_bf, w_down, preferred_element_type=jnp.float32)
    cot_bf = cot_out.astype(jnp.bfloat16)
    g_down = jnp.dot(act_bf.T, cot_bf, preferred_element_type=jnp.float32)
    grad_act = jnp.dot(cot_bf, w_down.T, preferred_element_type=jnp.float32)
    grad_hid = gelu_back(grad_act)[0].astype(jnp.bfloat16)
    g_up = jnp.dot(n_bf.T, grad_hid, preferred_element_type=jnp.float32)
    grad_n = jnp.dot(grad_hid, w_up.T, preferred_element_type=jnp.float32)
    return branch, rms_back(inv_rms, normed, grad_n), g_up, g_down


def attn_probs(qkv_seq):
    q_rows = qkv_seq[:, :, 0].astype(jnp.float32)
    k_rows = qkv_seq[:, :, 1].astype(jnp.float32)
    scores = jnp.einsum("qhe,khe->hqk", q_rows, k_rows) * SCORE_SCALE
    return jax.nn.softmax(scores, axis=-1)


def attn_seq_fwd(qkv_seq):
    prob_f = attn_probs(qkv_seq).astype(jnp.bfloat16).astype(jnp.float32)
    v_rows = qkv_seq[:, :, 2].astype(jnp.float32)
    return jnp.einsum("hqk,khe->qhe", prob_f, v_rows).astype(jnp.bfloat16)


def attn_seq_back(seq_args):
    qkv_seq, grad_o = seq_args
    attn_prob = attn_probs(qkv_seq)
    prob_f = attn_prob.astype(jnp.bfloat16).astype(jnp.float32)
    q_rows = qkv_seq[:, :, 0].astype(jnp.float32)
    k_rows = qkv_seq[:, :, 1].astype(jnp.float32)
    v_rows = qkv_seq[:, :, 2].astype(jnp.float32)
    grad_of = grad_o.astype(jnp.float32)
    grad_p = jnp.einsum("qhe,khe->hqk", grad_of, v_rows)
    grad_v = jnp.einsum("hqk,qhe->khe", prob_f, grad_of)
    grad_s = attn_prob * (grad_p - jnp.sum(grad_p * attn_prob, axis=-1, keepdims=True)) * SCORE_SCALE
    grad_s = grad_s.astype(jnp.bfloat16).astype(jnp.float32)
    grad_q = jnp.einsum("hqk,khe->qhe", grad_s, k_rows)
    grad_k = jnp.einsum("hqk,qhe->khe", grad_s, q_rows)
    return jnp.stack([grad_q, grad_k, grad_v], axis=2).astype(jnp.bfloat16)


def attn_block(x_in, cot_out, w_qkv, w_out):
    inv_rms, normed = rms_fwd(x_in)
    n_bf = normed.astype(jnp.bfloat16)
    qkv_mat = w_qkv.reshape(D, 3 * D)
    out_mat = w_out.reshape(D, D)
    qkv = jnp.dot(n_bf, qkv_mat, preferred_element_type=jnp.float32).astype(jnp.bfloat16)
    qkv = qkv.reshape(BATCH, SEQ, HEADS, 3, HEAD)
    attn_out = lax.map(attn_seq_fwd, qkv).reshape(TOKENS, D)
    branch = jnp.dot(attn_out, out_mat, preferred_element_type=jnp.float32)
    cot_bf = cot_out.astype(jnp.bfloat16)
    g_out = jnp.dot(attn_out.T, cot_bf, preferred_element_type=jnp.float32).reshape(HEADS, HEAD, D)
    grad_o = jnp.dot(cot_bf, out_mat.T, preferred_element_type=jnp.float32).astype(jnp.bfloat16)
    grad_o = grad_o.reshape(BATCH, SEQ, HEADS, HEAD)
    grad_qkv = lax.map(attn_seq_back, (qkv, grad_o)).reshape(TOKENS, 3 * D)
    g_qkv = jnp.dot(n_bf.T, grad_qkv, preferred_element_type=jnp.float32).reshape(D, HEADS, 3, HEAD)
    grad_n = jnp.dot(grad_qkv, qkv_mat.T, preferred_element_type=jnp.float32)
    return branch, rms_back(inv_rms, normed, grad_n), g_qkv, g_out


def reference(out_y1, out_y2, cot_y1, cot_y2, w_qkv, w_out, w_up, w_down):
    def layer_step(carry, weights):
        run_y1, run_y2, run_c1, run_c2 = carry
        layer_qkv, layer_out, layer_up, layer_down = weights
        g_branch, g_grad, g_up, g_down = mlp_block(run_y1, run_c2, layer_up, layer_down)
        low_x2 = run_y2 - g_branch
        run_c1 = run_c1 + g_grad
        f_branch, f_grad, g_qkv, g_out = attn_block(low_x2, run_c1, layer_qkv, layer_out)
        low_x1 = run_y1 - f_branch
        run_c2 = run_c2 + f_grad
        return (low_x1, low_x2, run_c1, run_c2), (g_qkv, g_out, g_up, g_down)

    init = (out_y1.reshape(TOKENS, D), out_y2.reshape(TOKENS, D), cot_y1.reshape(TOKENS, D), cot_y2.reshape(TOKENS, D))
    final, grads = lax.scan(layer_step, init, (w_qkv, w_out, w_up, w_down), reverse=True)
    return (final[0].reshape(BATCH, SEQ, D), final[1].reshape(BATCH, SEQ, D), final[2].reshape(BATCH, SEQ, D), final[3].reshape(BATCH, SEQ, D), grads[0], grads[1], grads[2], grads[3])
```

```python
import functools
import math

import jax
import jax.numpy as jnp
from jax import lax
from jax.experimental import pallas as pl
from jax.experimental.pallas import tpu as pltpu
from jax.sharding import PartitionSpec as P

F32, BF16 = jnp.float32, jnp.bfloat16
NORM_EPS = 1e-6
GELU_C = math.sqrt(2.0 / math.pi)
GELU_K = 0.044715
D = 1280
SEQ = 1024
HEAD = 80
HEADS_DEV = 2
QKV = 3 * HEAD * HEADS_DEV
OUT = HEAD * HEADS_DEV
FFD = 640
ROWS = 512
STEPS = 4
SCALE = 1.0 / math.sqrt(HEAD)
VMEM_CAP = 62 * 1024 * 1024


def dot(a, b, dims=((1,), (0,))):
    return lax.dot_general(a, b, (dims, ((), ())), preferred_element_type=F32)


NT = ((1,), (1,))
TN = ((0,), (0,))


def inv_rms(x):
    return lax.rsqrt(jnp.mean(x * x, axis=-1, keepdims=True) + NORM_EPS)


def gelu_pair(h):
    sq = h * h
    t = jnp.tanh(h * (GELU_C + (GELU_C * GELU_K) * sq))
    cdf = 0.5 + 0.5 * t
    act = h * cdf
    slope = cdf + (0.5 * h) * (1.0 - t * t) * (GELU_C + (3.0 * GELU_C * GELU_K) * sq)
    return act.astype(BF16), slope


def cost(flops, nbytes):
    return pl.CostEstimate(flops=int(flops), bytes_accessed=int(nbytes), transcendentals=0)


def any_spec():
    return pl.BlockSpec(memory_space=pl.ANY)


def params(**kw):
    return pltpu.CompilerParams(vmem_limit_bytes=VMEM_CAP, **kw)


def mlp_own_kernel(base, y1, c2, w1o, w1p, w2o, w2p, n_out, cot_out, act_out, dh_out, gp_out, np_out, w1, w2, sems):
    @pl.when(pl.program_id(0) == 0)
    def _():
        cps = [
            pltpu.make_async_copy(w1o, w1.at[:, pl.ds(0, FFD)], sems.at[0]),
            pltpu.make_async_copy(w1p, w1.at[:, pl.ds(FFD, FFD)], sems.at[1]),
            pltpu.make_async_copy(w2o, w2.at[pl.ds(0, FFD), :], sems.at[2]),
            pltpu.make_async_copy(w2p, w2.at[pl.ds(FFD, FFD), :], sems.at[3]),
        ]
        for cp in cps:
            cp.start()
        for cp in cps:
            cp.wait()

    y = y1[...]
    n_out[...] = (y * inv_rms(y)).astype(BF16)
    cot_out[...] = c2[...].astype(BF16)
    act, slope = gelu_pair(dot(n_out[...], w1[...]))
    act_out[...] = act
    dh = (dot(cot_out[...], w2[...], NT) * slope).astype(BF16)
    dh_out[...] = dh
    gp_out[...] = dot(act, w2[...])
    np_out[...] = dot(dh, w1[...], NT)


def mlp_own(core, y1, c2, w1o, w1p, w2o, w2p):
    half = STEPS * SEQ
    blocks = half // ROWS
    row_in = pl.BlockSpec((ROWS, D), lambda i, base: (base[0] * blocks + i, 0))
    row_out = pl.BlockSpec((ROWS, D), lambda i, base: (i, 0))
    return pl.pallas_call(
        mlp_own_kernel,
        name="mlp_own",
        grid_spec=pltpu.PrefetchScalarGridSpec(
            num_scalar_prefetch=1,
            grid=(blocks,),
            in_specs=[row_in, row_in] + [any_spec()] * 4,
            out_specs=[row_out] * 6,
            scratch_shapes=[
                pltpu.VMEM((D, 2 * FFD), BF16),
                pltpu.VMEM((2 * FFD, D), BF16),
                pltpu.SemaphoreType.DMA((4,)),
            ],
        ),
        out_shape=[jax.ShapeDtypeStruct((half, D), BF16)] * 4 + [jax.ShapeDtypeStruct((half, D), F32)] * 2,
        compiler_params=params(dimension_semantics=("arbitrary",)),
        cost_estimate=cost(4 * 2 * half * D * 2 * FFD, 120e6),
    )(core, y1, c2, w1o, w1p, w2o, w2p)


def grad_kernel(split_rows, a, b, dep, own, peer, acc, sems):
    i = pl.program_id(0)

    @pl.when(i == 0)
    def _():
        acc[...] = jnp.zeros_like(acc)

    acc[...] += dot(a[...], b[...], TN)

    @pl.when(i == pl.num_programs(0) - 1)
    def _():
        part = lambda k: acc.at[pl.ds(k * FFD, FFD), :] if split_rows else acc.at[:, pl.ds(k * FFD, FFD)]
        cps = [pltpu.make_async_copy(part(0), own, sems.at[0]), pltpu.make_async_copy(part(1), peer, sems.at[1])]
        for cp in cps:
            cp.start()
        for cp in cps:
            cp.wait()


def mlp_grad(split_rows, a, b, dep):
    half = STEPS * SEQ
    row = pl.BlockSpec((ROWS, D), lambda i: (i, 0))
    shape = (FFD, D) if split_rows else (D, FFD)
    return pl.pallas_call(
        functools.partial(grad_kernel, split_rows),
        name="mlp_grad",
        grid=(half // ROWS,),
        in_specs=[row, row, any_spec()],
        out_specs=[any_spec()] * 2,
        scratch_shapes=[pltpu.VMEM((D, 2 * FFD), F32), pltpu.SemaphoreType.DMA((2,))],
        out_shape=[jax.ShapeDtypeStruct(shape, F32)] * 2,
        compiler_params=params(dimension_semantics=("arbitrary",)),
        cost_estimate=cost(2 * half * D * 2 * FFD, 30e6),
    )(a, b, dep)


def mlp_rest_kernel(step, base, n_in, cot_in, y1, y2, c1, gp, np_, *refs):
    ws = refs[:12]
    x2_out, d1_out = refs[13:15]
    w1, w2, late, accg, accn, wsem, lsem, osem = refs[15:]
    i = pl.program_id(0)
    row = base[0] * (STEPS * SEQ) + step * SEQ + i * ROWS
    row = pl.multiple_of(row, ROWS)
    loc = pl.multiple_of(step * SEQ + i * ROWS, ROWS)
    out_row = pl.multiple_of(i * ROWS, ROWS)

    def w_copies(k):
        a1o, a1p, a2o, a2p = ws[4 * k : 4 * k + 4]
        return [
            pltpu.make_async_copy(a1o, w1.at[k, :, pl.ds(0, FFD)], wsem.at[k, 0]),
            pltpu.make_async_copy(a1p, w1.at[k, :, pl.ds(FFD, FFD)], wsem.at[k, 1]),
            pltpu.make_async_copy(a2o, w2.at[k, pl.ds(0, FFD), :], wsem.at[k, 2]),
            pltpu.make_async_copy(a2p, w2.at[k, pl.ds(FFD, FFD), :], wsem.at[k, 3]),
        ]

    late_copies = [
        pltpu.make_async_copy(src.at[pl.ds(at, ROWS), :], late.at[j], lsem.at[j])
        for j, (src, at) in enumerate(((gp, loc), (np_, loc), (y2, row), (c1, row), (y1, row)))
    ]
    outs = [
        pltpu.make_async_copy(accg, x2_out.at[pl.ds(out_row, ROWS), :], osem.at[0]),
        pltpu.make_async_copy(accn, d1_out.at[pl.ds(out_row, ROWS), :], osem.at[1]),
    ]

    @pl.when(i == 0)
    def _():
        for k in range(3):
            for cp in w_copies(k):
                cp.start()

    for cp in late_copies:
        cp.start()

    @pl.when(i > 0)
    def _():
        for cp in outs:
            cp.wait()

    def chunk(k):
        @pl.when(i == 0)
        def _():
            for kk in range(3):
                @pl.when(k == kk)
                def _():
                    for cp in w_copies(kk):
                        cp.wait()

        act, slope = gelu_pair(dot(n_in[...], w1[k]))
        dh = (dot(cot_in[...], w2[k], NT) * slope).astype(BF16)
        g = dot(act, w2[k])
        gn = dot(dh, w1[k], NT)
        return g, gn

    def body(k, _):
        g, gn = chunk(k)

        @pl.when(k == 0)
        def _():
            accg[...] = g
            accn[...] = gn

        @pl.when(k == 1)
        def _():
            accg[...] += g
            accn[...] += gn

        @pl.when(k == 2)
        def _():
            for cp in late_copies:
                cp.wait()
            late[0] = late[0] + g
            late[1] = late[1] + gn

        return 0

    lax.fori_loop(0, 3, body, 0)

    def finish(r, _):
        at = pl.ds(pl.multiple_of(r * 8, 8), 8)
        accg[at, :] = late[2, at, :] - (accg[at, :] + late[0, at, :])
        y = late[4, at, :]
        k = inv_rms(y)
        nf = y * k
        gn = accn[at, :] + late[1, at, :]
        accn[at, :] = late[3, at, :] + k * (gn - nf * jnp.mean(nf * gn, axis=-1, keepdims=True))
        return 0

    lax.fori_loop(0, ROWS // 8, finish, 0, unroll=8)
    for cp in outs:
        cp.start()

    @pl.when(i == pl.num_programs(0) - 1)
    def _():
        for cp in outs:
            cp.wait()


def mlp_rest(step, core, n_in, cot_in, y1, y2, c1, gp, np_, ws, dep):
    blocks = SEQ // ROWS
    row_in = pl.BlockSpec((ROWS, D), lambda i, base: (step * blocks + i, 0))
    return pl.pallas_call(
        functools.partial(mlp_rest_kernel, step),
        name="mlp_rest",
        grid_spec=pltpu.PrefetchScalarGridSpec(
            num_scalar_prefetch=1,
            grid=(blocks,),
            in_specs=[row_in, row_in] + [any_spec()] * 18,
            out_specs=[any_spec()] * 2,
            scratch_shapes=[
                pltpu.VMEM((3, D, 2 * FFD), BF16),
                pltpu.VMEM((3, 2 * FFD, D), BF16),
                pltpu.VMEM((5, ROWS, D), F32),
                pltpu.VMEM((ROWS, D), F32),
                pltpu.VMEM((ROWS, D), F32),
                pltpu.SemaphoreType.DMA((3, 4)),
                pltpu.SemaphoreType.DMA((5,)),
                pltpu.SemaphoreType.DMA((2,)),
            ],
        ),
        out_shape=[jax.ShapeDtypeStruct((SEQ, D), F32)] * 2,
        compiler_params=params(dimension_semantics=("arbitrary",)),
        cost_estimate=cost(12 * 2 * SEQ * D * 2 * FFD, 60e6),
    )(core, n_in, cot_in, y1, y2, c1, gp, np_, *ws, dep)


def attn_kernel(step, chained, base, x2o, x2p, d1o, d1p, wq, wo, *refs):
    refs = refs[5:] if chained else refs[1:]
    x2_out, d1_out, aq, ao, oT_out, fn_out = refs[:6]
    (xb, cb, n2, cot, qkvT, dqkvT, dOT, oT, kb, vb, dk, dv, fnb, accq, acco, isem, wsem, osem, asem) = refs[6:]
    i = pl.program_id(0)
    core = base[0]

    def in_copies(j):
        sx, sc = ((x2o, d1o), (x2p, d1p))[j]
        return [
            pltpu.make_async_copy(sx, xb.at[j], isem.at[j, 0]),
            pltpu.make_async_copy(sc, cb.at[j], isem.at[j, 1]),
        ]

    def out_copies(j):
        owner = core if j == 0 else 1 - core
        row = pl.multiple_of(owner * (STEPS * SEQ) + step * SEQ, SEQ)
        return [
            pltpu.make_async_copy(xb.at[j], x2_out.at[pl.ds(row, SEQ), :], wsem.at[j, 0]),
            pltpu.make_async_copy(cb.at[j], d1_out.at[pl.ds(row, SEQ), :], wsem.at[j, 1]),
        ]

    def res_copies(j):
        owner = core if j == 0 else 1 - core
        col = pl.multiple_of(owner * SEQ, SEQ)
        return [
            pltpu.make_async_copy(oT, oT_out.at[:, pl.ds(col, SEQ)], osem.at[0]),
            pltpu.make_async_copy(fnb, fn_out.at[owner], osem.at[1]),
        ]

    @pl.when(i == 0)
    def _():
        for j in range(2):
            for cp in in_copies(j):
                cp.start()
        if chained:
            cps = [pltpu.make_async_copy(aq, accq, asem.at[0]), pltpu.make_async_copy(ao, acco, asem.at[1])]
            for cp in cps:
                cp.start()
            for cp in cps:
                cp.wait()
        else:
            accq[...] = jnp.zeros_like(accq)
            acco[...] = jnp.zeros_like(acco)

    for j in range(2):
        @pl.when(i == j)
        def _():
            for cp in in_copies(j):
                cp.wait()
            for cp in out_copies(j):
                cp.start()

    x = xb[i]
    n2[...] = (x * inv_rms(x)).astype(BF16)
    cot[...] = cb[i].astype(BF16)
    qkvT[...] = dot(wq[...], n2[...], NT).astype(BF16)
    dO = dot(cot[...], wo[...], NT).astype(BF16)
    dOT[...] = dO.T

    @pl.when(i == 1)
    def _():
        for cp in res_copies(0):
            cp.wait()

    def head(h, _):
        at = pl.multiple_of(h * (3 * HEAD), 16)
        oat = pl.multiple_of(h * HEAD, 16)
        kT = qkvT[pl.ds(at + HEAD, HEAD), :]
        vT = qkvT[pl.ds(at + 2 * HEAD, HEAD), :]
        kb[...] = kT.T
        vb[...] = vT.T
        for qb in range(SEQ // ROWS):
            cols = pl.ds(qb * ROWS, ROWS)
            qT = qkvT[pl.ds(at, HEAD), cols]
            gT = dOT[pl.ds(oat, HEAD), cols]
            s = dot(kb[...], qT)
            m = jnp.max(s, axis=0, keepdims=True)
            p = jnp.exp2((s - m) * (SCALE * math.log2(math.e)))
            p = p * (1.0 / jnp.sum(p, axis=0, keepdims=True))
            pb = p.astype(BF16)
            dp = dot(vb[...], gT)
            r = jnp.sum(dp * p, axis=0, keepdims=True)
            ds = (p * (dp - r) * SCALE).astype(BF16)
            oT[pl.ds(oat, HEAD), cols] = dot(qkvT[pl.ds(at + 2 * HEAD, HEAD), :], pb).astype(BF16)
            dvp = dot(pb, gT.T)
            dqkvT[pl.ds(at, HEAD), cols] = dot(qkvT[pl.ds(at + HEAD, HEAD), :], ds).astype(BF16)
            dkp = dot(ds, qT.T)
            if qb == 0:
                dv[...] = dvp
                dk[...] = dkp
            else:
                dqkvT[pl.ds(at + 2 * HEAD, HEAD), :] = (dv[...] + dvp).astype(BF16).T
                dqkvT[pl.ds(at + HEAD, HEAD), :] = (dk[...] + dkp).astype(BF16).T
        return 0

    lax.fori_loop(0, HEADS_DEV, head, 0)
    fnb[...] = dot(dqkvT[...], wq[...], TN).astype(BF16)
    for j in range(2):
        @pl.when(i == j)
        def _():
            for cp in res_copies(j):
                cp.start()
    accq[...] += dot(dqkvT[...], n2[...])
    acco[...] += dot(oT[...], cot[...])

    @pl.when(i == 1)
    def _():
        cps = [pltpu.make_async_copy(accq, aq, asem.at[0]), pltpu.make_async_copy(acco, ao, asem.at[1])]
        for cp in cps:
            cp.start()
        for cp in cps + res_copies(1) + out_copies(0) + out_copies(1):
            cp.wait()


def attn(step, core, x2o, x2p, d1o, d1p, wq, wo, dep, chain):
    full = jax.ShapeDtypeStruct((2 * STEPS * SEQ, D), F32)
    whole = lambda shape: pl.BlockSpec(shape, lambda i, base: (0, 0))
    chained = chain is not None
    ins = [core, x2o, x2p, d1o, d1p, wq, wo, dep] + (list(chain) if chained else [])
    return pl.pallas_call(
        functools.partial(attn_kernel, step, chained),
        name="attn",
        grid_spec=pltpu.PrefetchScalarGridSpec(
            num_scalar_prefetch=1,
            grid=(2,),
            in_specs=[any_spec()] * 4 + [whole((QKV, D)), whole((OUT, D))] + [any_spec()] * (5 if chained else 1),
            out_specs=[any_spec()] * 6,
            scratch_shapes=[
                pltpu.VMEM((2, SEQ, D), F32),
                pltpu.VMEM((2, SEQ, D), F32),
                pltpu.VMEM((SEQ, D), BF16),
                pltpu.VMEM((SEQ, D), BF16),
                pltpu.VMEM((QKV, SEQ), BF16),
                pltpu.VMEM((QKV, SEQ), BF16),
                pltpu.VMEM((OUT, SEQ), BF16),
                pltpu.VMEM((OUT, SEQ), BF16),
                pltpu.VMEM((SEQ, HEAD), BF16),
                pltpu.VMEM((SEQ, HEAD), BF16),
                pltpu.VMEM((SEQ, HEAD), F32),
                pltpu.VMEM((SEQ, HEAD), F32),
                pltpu.VMEM((SEQ, D), BF16),
                pltpu.VMEM((QKV, D), F32),
                pltpu.VMEM((OUT, D), F32),
                pltpu.SemaphoreType.DMA((2, 2)),
                pltpu.SemaphoreType.DMA((2, 2)),
                pltpu.SemaphoreType.DMA((2,)),
                pltpu.SemaphoreType.DMA((2,)),
            ],
        ),
        out_shape=[
            full,
            full,
            jax.ShapeDtypeStruct((QKV, D), F32),
            jax.ShapeDtypeStruct((OUT, D), F32),
            jax.ShapeDtypeStruct((OUT, 2 * SEQ), BF16),
            jax.ShapeDtypeStruct((2, SEQ, D), BF16),
        ],
        input_output_aliases={8 + k: k for k in range(4)} if chained else {},
        compiler_params=params(dimension_semantics=("arbitrary",)),
        cost_estimate=cost(24e9, 60e6),
    )(*ins)


def out_proj_kernel(y1, oT, wo, *refs):
    refs[-1][...] = y1[...] - dot(oT[...], wo[...], TN)


def out_proj(step, y1, oT, wo, dep, chain):
    per = SEQ // ROWS
    chained = chain is not None
    row = pl.BlockSpec((ROWS, D), lambda i: ((i // per) * (STEPS * per) + step * per + i % per, 0))
    return pl.pallas_call(
        out_proj_kernel,
        name="out_proj",
        grid=(2 * per,),
        in_specs=[row, pl.BlockSpec((8 * OUT, ROWS), lambda i: (0, i)), pl.BlockSpec((8 * OUT, D), lambda i: (0, 0)), any_spec()]
        + [any_spec()] * (1 if chained else 0),
        out_specs=row,
        out_shape=jax.ShapeDtypeStruct((2 * STEPS * SEQ, D), F32),
        input_output_aliases={4: 0} if chained else {},
        compiler_params=params(dimension_semantics=("arbitrary",)),
        cost_estimate=cost(2 * 2 * SEQ * D * D, 30e6),
    )(y1, oT, wo, dep, *([chain] if chained else []))


def norm_back_kernel(per, base, x2o, x2p, f, c2, *refs):
    out = refs[-1]

    def run(x_ref):
        def rows(r, _):
            at = pl.ds(pl.multiple_of(r * 16, 16), 16)
            x = x_ref[at, :]
            k = inv_rms(x)
            nf = x * k
            g = f[at, :].astype(F32)
            out[at, :] = c2[at, :] + k * (g - nf * jnp.mean(nf * g, axis=-1, keepdims=True))
            return 0

        lax.fori_loop(0, ROWS // 16, rows, 0, unroll=4)

    @pl.when(pl.program_id(0) < per)
    def _():
        run(x2o)

    @pl.when(pl.program_id(0) >= per)
    def _():
        run(x2p)


def norm_back(step, core, x2o, x2p, f, c2, dep, chain):
    per = SEQ // ROWS
    chained = chain is not None
    own = pl.BlockSpec((ROWS, D), lambda i, base: (jnp.minimum(i, per - 1), 0))
    peer = pl.BlockSpec((ROWS, D), lambda i, base: (jnp.maximum(i - per, 0), 0))

    def at(i, base, stride, off):
        owner = jnp.where(i < per, base[0], 1 - base[0])
        return (owner * (stride * per) + off * per + i % per, 0)

    row = pl.BlockSpec((ROWS, D), lambda i, base: at(i, base, STEPS, step))
    frow = pl.BlockSpec((ROWS, D), lambda i, base: at(i, base, 1, 0))
    return pl.pallas_call(
        functools.partial(norm_back_kernel, per),
        name="norm_back",
        grid_spec=pltpu.PrefetchScalarGridSpec(
            num_scalar_prefetch=1,
            grid=(2 * per,),
            in_specs=[own, peer, frow, row, any_spec()] + [any_spec()] * (1 if chained else 0),
            out_specs=row,
        ),
        out_shape=jax.ShapeDtypeStruct((2 * STEPS * SEQ, D), F32),
        input_output_aliases={6: 0} if chained else {},
        compiler_params=params(dimension_semantics=("arbitrary",)),
        cost_estimate=cost(4e9, 40e6),
    )(core, x2o, x2p, f, c2, dep, *([chain] if chained else []))


def solution(mesh):
    act_spec = P("dp", None, None)
    weight_specs = (P(None, None, "tp", None, None), P(None, "tp", None, None), P(None, None, "tp"), P(None, "tp", None))
    grad_specs = (P("dp", None, "tp", None, None), P("dp", "tp", None, None), P("dp", None, "tp"), P("dp", "tp", None))

    pair_core = [(t, t ^ 1) for t in range(8)]
    pair_a = [(t, t ^ (4 if t & 1 else 2)) for t in range(8)]
    pair_b = [(t, t ^ (2 if t & 1 else 4)) for t in range(8)]

    def swap(x, pairs):
        return lax.ppermute(x, "tp", pairs)

    def local_backward(out_y1, out_y2, cot_y1, cot_y2, w_qkv, w_out, w_up, w_down):
        core = lax.axis_index("tp") & 1
        base = core.reshape(1).astype(jnp.int32)
        flat = lambda z: z.reshape(2 * STEPS * SEQ, D)
        y1, y2, c1, c2 = flat(out_y1), flat(out_y2), flat(cot_y1), flat(cot_y2)
        w1, w2 = w_up[0], w_down[0]
        wq = jnp.transpose(w_qkv[0], (1, 2, 3, 0)).reshape(QKV, D)
        wo = w_out[0].reshape(OUT, D)

        w1p, w2p = swap(w1, pair_core), swap(w2, pair_core)
        w1a, w2a = swap(w1, pair_a), swap(w2, pair_a)
        w1b, w2b = swap(w1, pair_b), swap(w2, pair_b)
        n_all, cot_all, act, dh, gp, np_ = mlp_own(base, y1, c2, w1, w1p, w2, w2p)
        w1a, w2a, w1b, w2b, np_ = lax.optimization_barrier((w1a, w2a, w1b, w2b, np_))
        w1d, w2d = swap(w1b, pair_a), swap(w2b, pair_a)
        d1o, d1p = mlp_grad(False, n_all, dh, np_)
        rest = []
        for u, d in ((w1a, w2a), (w1b, w2b)):
            rest += [u, swap(u, pair_core), d, swap(d, pair_core)]
        w1d, w2d, d1o = lax.optimization_barrier((w1d, w2d, d1o))
        rest += [w1d, swap(w1d, pair_core), w2d, swap(w2d, pair_core)]
        wo_all = lax.all_gather(wo, "tp", axis=0, tiled=True)

        x2s, d1s = [None] * STEPS, [None] * STEPS
        ots, fns = [None] * STEPS, [None] * STEPS
        chain = x1 = dx2 = None

        def mlp(s, dep):
            x, d = mlp_rest(s, base, n_all, cot_all, y1, y2, c1, gp, np_, rest, dep)
            x2s[s], d1s[s] = (x, swap(x, pair_core)), (d, swap(d, pair_core))
            return x

        def att(s, dep):
            nonlocal chain
            *chain, oT, fn = attn(s, base, *x2s[s], *d1s[s], wq, wo, dep, chain)
            ots[s] = lax.all_gather(oT, "tp", axis=0, tiled=True)
            if s:
                fn, fns[s - 1] = lax.optimization_barrier((fn, fns[s - 1]))
            fns[s] = lax.psum(fn.reshape(2 * SEQ, D), "tp")
            return chain[3]

        def proj(s, dep):
            nonlocal x1
            x1 = out_proj(s, y1, ots[s], wo_all, dep, x1)
            return x1

        def back(s, dep):
            nonlocal dx2
            dx2 = norm_back(s, base, *x2s[s], fns[s], c2, dep, dx2)
            return dx2

        t = mlp(0, d1o)
        d2o, d2p = mlp_grad(True, act, cot_all, t)
        g_up = d1o + swap(d1p, pair_core)
        g_down = d2o + swap(d2p, pair_core)
        t = att(0, d2o)
        t = mlp(1, t)
        t = proj(0, t)
        t = att(1, t)
        t = mlp(2, t)
        t = back(0, t)
        t = proj(1, t)
        t = att(2, t)
        t = mlp(3, t)
        t = back(1, t)
        t = proj(2, t)
        t = att(3, t)
        t = back(2, t)
        t = proj(3, t)
        back(3, t)

        x2, dx1, aq, ao = chain
        full = lambda z: z.reshape(2 * STEPS, SEQ, D)
        g_qkv = jnp.transpose(aq.reshape(HEADS_DEV, 3, HEAD, D), (3, 0, 1, 2))
        g_out = ao.reshape(HEADS_DEV, HEAD, D)
        return full(x1), full(x2), full(dx1), full(dx2), g_qkv[None], g_out[None], g_up[None], g_down[None]

    return jax.shard_map(
        local_backward,
        mesh=mesh,
        in_specs=(act_spec,) * 4 + weight_specs,
        out_specs=(act_spec,) * 4 + grad_specs,
        check_vma=False,
    )
```

```python
import functools
import math

import jax
import jax.numpy as jnp
from jax import lax
from jax.experimental import pallas as pl
from jax.experimental.pallas import tpu as pltpu
from jax.sharding import PartitionSpec as P

F32, BF16 = jnp.float32, jnp.bfloat16
NORM_EPS = 1e-6
GELU_C = math.sqrt(2.0 / math.pi)
GELU_K = 0.044715
D = 1280
SEQ = 1024
HEAD = 80
HEADS_DEV = 2
QKV = 3 * HEAD * HEADS_DEV
OUT = HEAD * HEADS_DEV
FFD = 640
ROWS = 512
STEPS = 4
SCALE = 1.0 / math.sqrt(HEAD)
VMEM_CAP = 62 * 1024 * 1024


def dot(a, b, dims=((1,), (0,))):
    return lax.dot_general(a, b, (dims, ((), ())), preferred_element_type=F32)


NT = ((1,), (1,))
TN = ((0,), (0,))


def inv_rms(x):
    return lax.rsqrt(jnp.mean(x * x, axis=-1, keepdims=True) + NORM_EPS)


def gelu_pair(h):
    sq = h * h
    t = jnp.tanh(h * (GELU_C + (GELU_C * GELU_K) * sq))
    cdf = 0.5 + 0.5 * t
    act = h * cdf
    slope = cdf + (0.5 * h) * (1.0 - t * t) * (GELU_C + (3.0 * GELU_C * GELU_K) * sq)
    return act.astype(BF16), slope


def cost(flops, nbytes):
    return pl.CostEstimate(flops=int(flops), bytes_accessed=int(nbytes), transcendentals=0)


def any_spec():
    return pl.BlockSpec(memory_space=pl.ANY)


def params(**kw):
    return pltpu.CompilerParams(vmem_limit_bytes=VMEM_CAP, **kw)


def mlp_own_kernel(base, y1, c2, w1o, w1p, w2o, w2p, n_out, cot_out, act_out, dh_out, gp_out, np_out, w1, w2, sems):
    @pl.when(pl.program_id(0) == 0)
    def _():
        cps = [
            pltpu.make_async_copy(w1o, w1.at[:, pl.ds(0, FFD)], sems.at[0]),
            pltpu.make_async_copy(w1p, w1.at[:, pl.ds(FFD, FFD)], sems.at[1]),
            pltpu.make_async_copy(w2o, w2.at[pl.ds(0, FFD), :], sems.at[2]),
            pltpu.make_async_copy(w2p, w2.at[pl.ds(FFD, FFD), :], sems.at[3]),
        ]
        for cp in cps:
            cp.start()
        for cp in cps:
            cp.wait()

    cot = c2[...].astype(BF16)
    cot_out[...] = cot
    da = dot(cot, w2[...], NT)
    y = y1[...]
    n = (y * inv_rms(y)).astype(BF16)
    n_out[...] = n
    act, slope = gelu_pair(dot(n, w1[...]))
    act_out[...] = act
    dh = (da * slope).astype(BF16)
    dh_out[...] = dh
    gp_out[...] = dot(act, w2[...])
    np_out[...] = dot(dh, w1[...], NT)


def mlp_own(core, y1, c2, w1o, w1p, w2o, w2p):
    half = STEPS * SEQ
    blocks = half // ROWS
    row_in = pl.BlockSpec((ROWS, D), lambda i, base: (base[0] * blocks + i, 0))
    row_out = pl.BlockSpec((ROWS, D), lambda i, base: (i, 0))
    return pl.pallas_call(
        mlp_own_kernel,
        name="mlp_own",
        grid_spec=pltpu.PrefetchScalarGridSpec(
            num_scalar_prefetch=1,
            grid=(blocks,),
            in_specs=[row_in, row_in] + [any_spec()] * 4,
            out_specs=[row_out] * 6,
            scratch_shapes=[
                pltpu.VMEM((D, 2 * FFD), BF16),
                pltpu.VMEM((2 * FFD, D), BF16),
                pltpu.SemaphoreType.DMA((4,)),
            ],
        ),
        out_shape=[jax.ShapeDtypeStruct((half, D), BF16)] * 4 + [jax.ShapeDtypeStruct((half, D), F32)] * 2,
        compiler_params=params(dimension_semantics=("arbitrary",)),
        cost_estimate=cost(4 * 2 * half * D * 2 * FFD, 120e6),
    )(core, y1, c2, w1o, w1p, w2o, w2p)


def grad_kernel(split_rows, a, b, dep, own, peer, acc, sems):
    i = pl.program_id(0)

    @pl.when(i == 0)
    def _():
        acc[...] = jnp.zeros_like(acc)

    acc[...] += dot(a[...], b[...], TN)

    @pl.when(i == pl.num_programs(0) - 1)
    def _():
        part = lambda k: acc.at[pl.ds(k * FFD, FFD), :] if split_rows else acc.at[:, pl.ds(k * FFD, FFD)]
        cps = [pltpu.make_async_copy(part(0), own, sems.at[0]), pltpu.make_async_copy(part(1), peer, sems.at[1])]
        for cp in cps:
            cp.start()
        for cp in cps:
            cp.wait()


def mlp_grad(split_rows, a, b, dep):
    half = STEPS * SEQ
    row = pl.BlockSpec((SEQ, D), lambda i: (i, 0))
    shape = (FFD, D) if split_rows else (D, FFD)
    return pl.pallas_call(
        functools.partial(grad_kernel, split_rows),
        name="mlp_grad",
        grid=(half // SEQ,),
        in_specs=[row, row, any_spec()],
        out_specs=[any_spec()] * 2,
        scratch_shapes=[pltpu.VMEM((D, 2 * FFD), F32), pltpu.SemaphoreType.DMA((2,))],
        out_shape=[jax.ShapeDtypeStruct(shape, F32)] * 2,
        compiler_params=params(dimension_semantics=("arbitrary",)),
        cost_estimate=cost(2 * half * D * 2 * FFD, 30e6),
    )(a, b, dep)


def mlp_rest_kernel(step, chunks, resumed, final, base, n_in, cot_in, y1, y2, c1, gp, np_, *refs):
    ws = refs[: 4 * chunks]
    refs = refs[4 * chunks :]
    part = refs[:2]
    refs = refs[2:] if resumed else refs
    out_g, out_n = refs[1:3]
    w1, w2, late, accg, accn, wsem, lsem, osem = refs[3:]
    i = pl.program_id(0)
    row = pl.multiple_of(base[0] * (STEPS * SEQ) + step * SEQ + i * ROWS, ROWS)
    loc = pl.multiple_of(step * SEQ + i * ROWS, ROWS)
    out_row = pl.multiple_of(i * ROWS, ROWS)

    def w_copies(k):
        a1o, a1p, a2o, a2p = ws[4 * k : 4 * k + 4]
        return [
            pltpu.make_async_copy(a1o, w1.at[k, :, pl.ds(0, FFD)], wsem.at[k, 0]),
            pltpu.make_async_copy(a1p, w1.at[k, :, pl.ds(FFD, FFD)], wsem.at[k, 1]),
            pltpu.make_async_copy(a2o, w2.at[k, pl.ds(0, FFD), :], wsem.at[k, 2]),
            pltpu.make_async_copy(a2p, w2.at[k, pl.ds(FFD, FFD), :], wsem.at[k, 3]),
        ]

    def start(cps):
        for cp in cps:
            cp.start()

    def wait(cps):
        for cp in cps:
            cp.wait()

    srcs = [(np_, loc), (y1, row), (c1, row), (gp, loc), (y2, row)] if final else []
    if resumed:
        srcs += [(part[0], out_row), (part[1], out_row)]
    late_copies = [
        pltpu.make_async_copy(src.at[pl.ds(at, ROWS), :], late.at[j], lsem.at[j]) for j, (src, at) in enumerate(srcs)
    ]
    outs = [
        pltpu.make_async_copy(accg, out_g.at[pl.ds(out_row, ROWS), :], osem.at[0]),
        pltpu.make_async_copy(accn, out_n.at[pl.ds(out_row, ROWS), :], osem.at[1]),
    ]

    def arrive(k):
        @pl.when(i == 0)
        def _():
            if k == 0:
                start(w_copies(0))
            wait(w_copies(k))
            if k + 1 < chunks:
                start(w_copies(k + 1))

    for k in range(chunks):
        arrive(k)
        if k == chunks - 1:
            start(late_copies)
        if k == min(1, chunks - 1):
            @pl.when(i > 0)
            def _():
                wait(outs)
        last = final and k == chunks - 1
        act, slope = gelu_pair(dot(n_in[...], w1[k]))
        dh = (dot(cot_in[...], w2[k], NT) * slope).astype(BF16)
        if last:
            wait(late_copies)
        gn = dot(dh, w1[k], NT)
        if not last:
            accn[...] = gn if k == 0 else accn[...] + gn
            g = dot(act, w2[k])
            accg[...] = g if k == 0 else accg[...] + g
            continue
        prev_n = late[6] if resumed else accn[...]
        gn = prev_n + (late[0] + gn)
        y = late[1]
        r = inv_rms(y)
        nf = y * r
        accn[...] = late[2] + r * (gn - nf * jnp.mean(nf * gn, axis=-1, keepdims=True))
        prev_g = late[5] if resumed else accg[...]
        accg[...] = late[4] - (prev_g + (late[3] + dot(act, w2[k])))
    start(outs)

    @pl.when(i == pl.num_programs(0) - 1)
    def _():
        wait(outs)


def mlp_rest(step, core, n_in, cot_in, y1, y2, c1, gp, np_, ws, part, dep, final):
    blocks = SEQ // ROWS
    chunks = len(ws) // 4
    resumed = part is not None
    lates = (5 if final else 0) + (2 if resumed else 0)
    row_in = pl.BlockSpec((ROWS, D), lambda i, base: (step * blocks + i, 0))
    ins = [y1, y2, c1, gp, np_, *ws, *(part or ()), dep]
    return pl.pallas_call(
        functools.partial(mlp_rest_kernel, step, chunks, resumed, final),
        name="mlp_rest",
        grid_spec=pltpu.PrefetchScalarGridSpec(
            num_scalar_prefetch=1,
            grid=(blocks,),
            in_specs=[row_in, row_in] + [any_spec()] * len(ins),
            out_specs=[any_spec()] * 2,
            scratch_shapes=[
                pltpu.VMEM((chunks, D, 2 * FFD), BF16),
                pltpu.VMEM((chunks, 2 * FFD, D), BF16),
                pltpu.VMEM((max(lates, 1), ROWS, D), F32),
                pltpu.VMEM((ROWS, D), F32),
                pltpu.VMEM((ROWS, D), F32),
                pltpu.SemaphoreType.DMA((chunks, 4)),
                pltpu.SemaphoreType.DMA((max(lates, 1),)),
                pltpu.SemaphoreType.DMA((2,)),
            ],
        ),
        out_shape=[jax.ShapeDtypeStruct((SEQ, D), F32)] * 2,
        compiler_params=params(dimension_semantics=("arbitrary",)),
        cost_estimate=cost(chunks * 4 * 2 * SEQ * D * 2 * FFD, 60e6),
    )(core, n_in, cot_in, *ins)


PARTS = 2


def attn_kernel(step, peer, chained, base, x2, d1, wq, wo, *refs):
    nin = (0 if peer else 2) + (4 if chained else 0) + 1
    fr = None if peer else refs[0]
    refs = refs[nin:]
    nout = 6 if peer else 7
    x2_out, d1_out, aq, ao, oT_out = refs[:5]
    fouts = refs[5:nout]
    scr = refs[nout:]
    xb, cb, n2, cot, qkvT, dqkvT, dOT, oT, kb, vb, dk, dv, fnb, accq, acco, isem, wsem, osem, asem = scr[:19]
    frb, frsem = (None, None) if peer else scr[19:]
    owner = 1 - base[0] if peer else base[0]
    row = pl.multiple_of(owner * (STEPS * SEQ) + step * SEQ, SEQ)
    size = SEQ // PARTS

    def start(cps):
        for cp in cps:
            cp.start()

    def wait(cps):
        for cp in cps:
            cp.wait()

    def in_copy(src, dst, which, r):
        at = pl.ds(r * size, size)
        return pltpu.make_async_copy(src.at[at, :], dst.at[at, :], isem.at[which, r])

    xin = [in_copy(x2, xb, 0, r) for r in range(PARTS)]
    cin = [in_copy(d1, cb, 1, r) for r in range(PARTS)]
    echo = [
        pltpu.make_async_copy(xb, x2_out.at[pl.ds(row, SEQ), :], wsem.at[0]),
        pltpu.make_async_copy(cb, d1_out.at[pl.ds(row, SEQ), :], wsem.at[1]),
    ]
    acc_out = [pltpu.make_async_copy(accq, aq, asem.at[0]), pltpu.make_async_copy(acco, ao, asem.at[1])]
    col = pl.multiple_of(owner * SEQ, SEQ)
    o_out = pltpu.make_async_copy(oT, oT_out.at[:, pl.ds(col, SEQ)], osem.at[0])
    queue = xin + cin
    start(queue[:2])
    if chained:
        acc_in = [pltpu.make_async_copy(aq, accq, asem.at[0]), pltpu.make_async_copy(ao, acco, asem.at[1])]
    for r in range(PARTS):
        xin[r].wait()
        start(queue[r + 2 : r + 3])
        rows = pl.ds(r * size, size)
        x = xb[rows, :]
        n = (x * inv_rms(x)).astype(BF16)
        n2[rows, :] = n
        qkvT[:, rows] = dot(wq[...], n, NT).astype(BF16)
    for r in range(PARTS):
        cin[r].wait()
        start(queue[r + PARTS + 2 : r + PARTS + 3])
        rows = pl.ds(r * size, size)
        c = cb[rows, :].astype(BF16)
        cot[rows, :] = c
        dOT[:, rows] = dot(c, wo[...], NT).astype(BF16).T
    start(echo)
    if chained:
        start(acc_in)
    if not peer:
        fr_in = pltpu.make_async_copy(fr, frb, frsem.at[0])
        fr_in.start()

    def head(h, _):
        at = pl.multiple_of(h * (3 * HEAD), 16)
        oat = pl.multiple_of(h * HEAD, 16)
        kb[...] = qkvT[pl.ds(at + HEAD, HEAD), :].T
        vb[...] = qkvT[pl.ds(at + 2 * HEAD, HEAD), :].T
        for qb in range(SEQ // ROWS):
            cols = pl.ds(qb * ROWS, ROWS)
            qT = qkvT[pl.ds(at, HEAD), cols]
            gT = dOT[pl.ds(oat, HEAD), cols]
            s = dot(kb[...], qT)
            m = jnp.max(s, axis=0, keepdims=True)
            p = jnp.exp2((s - m) * (SCALE * math.log2(math.e)))
            p = p * (1.0 / jnp.sum(p, axis=0, keepdims=True))
            pb = p.astype(BF16)
            dp = dot(vb[...], gT)
            r = jnp.sum(dp * p, axis=0, keepdims=True)
            ds = (p * (dp - r) * SCALE).astype(BF16)
            oT[pl.ds(oat, HEAD), cols] = dot(qkvT[pl.ds(at + 2 * HEAD, HEAD), :], pb).astype(BF16)
            dvp = dot(pb, gT.T)
            dqkvT[pl.ds(at, HEAD), cols] = dot(qkvT[pl.ds(at + HEAD, HEAD), :], ds).astype(BF16)
            dkp = dot(ds, qT.T)
            if qb == 0:
                dv[...] = dvp
                dk[...] = dkp
            else:
                dqkvT[pl.ds(at + 2 * HEAD, HEAD), :] = (dv[...] + dvp).astype(BF16).T
                dqkvT[pl.ds(at + HEAD, HEAD), :] = (dk[...] + dkp).astype(BF16).T
        return 0

    lax.fori_loop(0, HEADS_DEV, head, 0)
    o_out.start()
    if peer:
        fnb[...] = dot(dqkvT[...], wq[...], TN).astype(BF16)
        f_out = [pltpu.make_async_copy(fnb, fouts[0], osem.at[1])]
    else:
        fr_in.wait()
        fnb[...] = dot(dqkvT[...], wq[...], TN) + frb[...].astype(F32)
        half = SEQ // 2
        go = pl.multiple_of((1 - base[1]) * half, half)
        stay = pl.multiple_of(base[1] * half, half)
        frb[pl.ds(0, half), :] = fnb[pl.ds(go, half), :].astype(BF16)
        f_out = [
            pltpu.make_async_copy(frb.at[pl.ds(0, half), :], fouts[0], osem.at[1]),
            pltpu.make_async_copy(fnb.at[pl.ds(stay, half), :], fouts[1], osem.at[2]),
        ]
    start(f_out)
    dq = dot(dqkvT[...], n2[...])
    do = dot(oT[...], cot[...])
    if chained:
        wait(acc_in)
        accq[...] += dq
        acco[...] += do
    else:
        accq[...] = dq
        acco[...] = do
    start(acc_out)
    wait(acc_out + f_out + [o_out] + echo)


def attn(step, peer, core, x2, d1, wq, wo, fr, oT, dep, chain):
    full = jax.ShapeDtypeStruct((2 * STEPS * SEQ, D), F32)
    whole = lambda shape: pl.BlockSpec(shape, lambda i, base: (0, 0))
    chained = chain is not None
    ins = [core, x2, d1, wq, wo] + ([] if peer else [fr, oT])
    first = len(ins)
    ins += (list(chain) if chained else []) + [dep]
    alias = {first + k: k for k in range(4)} if chained else {}
    if not peer:
        alias[6] = 4
    half = SEQ // 2
    if peer:
        fshapes = [jax.ShapeDtypeStruct((SEQ, D), BF16)]
    else:
        fshapes = [jax.ShapeDtypeStruct((half, D), BF16), jax.ShapeDtypeStruct((half, D), F32)]
    return pl.pallas_call(
        functools.partial(attn_kernel, step, peer, chained),
        name="attn",
        grid_spec=pltpu.PrefetchScalarGridSpec(
            num_scalar_prefetch=1,
            grid=(1,),
            in_specs=[any_spec()] * 2 + [whole((QKV, D)), whole((OUT, D))] + [any_spec()] * (len(ins) - 5),
            out_specs=[any_spec()] * (5 + len(fshapes)),
            scratch_shapes=[
                pltpu.VMEM((SEQ, D), F32),
                pltpu.VMEM((SEQ, D), F32),
                pltpu.VMEM((SEQ, D), BF16),
                pltpu.VMEM((SEQ, D), BF16),
                pltpu.VMEM((QKV, SEQ), BF16),
                pltpu.VMEM((QKV, SEQ), BF16),
                pltpu.VMEM((OUT, SEQ), BF16),
                pltpu.VMEM((OUT, SEQ), BF16),
                pltpu.VMEM((SEQ, HEAD), BF16),
                pltpu.VMEM((SEQ, HEAD), BF16),
                pltpu.VMEM((SEQ, HEAD), F32),
                pltpu.VMEM((SEQ, HEAD), F32),
                pltpu.VMEM((SEQ, D), BF16 if peer else F32),
                pltpu.VMEM((QKV, D), F32),
                pltpu.VMEM((OUT, D), F32),
                pltpu.SemaphoreType.DMA((2, PARTS)),
                pltpu.SemaphoreType.DMA((2,)),
                pltpu.SemaphoreType.DMA((3,)),
                pltpu.SemaphoreType.DMA((2,)),
            ]
            + ([] if peer else [pltpu.VMEM((SEQ, D), BF16), pltpu.SemaphoreType.DMA((1,))]),
        ),
        out_shape=[
            full,
            full,
            jax.ShapeDtypeStruct((QKV, D), F32),
            jax.ShapeDtypeStruct((OUT, D), F32),
            jax.ShapeDtypeStruct((OUT, 2 * SEQ), BF16),
        ]
        + fshapes,
        input_output_aliases=alias,
        compiler_params=params(dimension_semantics=("arbitrary",)),
        cost_estimate=cost(15e9, 30e6),
    )(*ins)


def out_proj_kernel(chained, pos, y1, *refs):
    os_, ws = refs[:8], refs[8:16]
    refs = refs[18:] if chained else refs[17:]
    x1, oT, wo, sems = refs

    @pl.when(pl.program_id(0) == 0)
    def _():
        cps = []
        for k in range(8):
            at = pl.multiple_of(pos[k] * OUT, OUT)
            cps.append(pltpu.make_async_copy(os_[k], oT.at[pl.ds(at, OUT), :], sems.at[0, k]))
            cps.append(pltpu.make_async_copy(ws[k], wo.at[pl.ds(at, OUT), :], sems.at[1, k]))
        for cp in cps:
            cp.start()
        for cp in cps:
            cp.wait()

    col = pl.multiple_of(pl.program_id(0) * ROWS, ROWS)
    x1[...] = y1[...] - dot(oT[:, pl.ds(col, ROWS)], wo[...], TN)


def out_proj(step, pos, y1, os_, ws, dep, chain):
    per = SEQ // ROWS
    chained = chain is not None
    row = pl.BlockSpec((ROWS, D), lambda i, pos: ((i // per) * (STEPS * per) + step * per + i % per, 0))
    return pl.pallas_call(
        functools.partial(out_proj_kernel, chained),
        name="out_proj",
        grid_spec=pltpu.PrefetchScalarGridSpec(
            num_scalar_prefetch=1,
            grid=(2 * per,),
            in_specs=[row] + [any_spec()] * (18 if chained else 17),
            out_specs=row,
            scratch_shapes=[
                pltpu.VMEM((8 * OUT, 2 * SEQ), BF16),
                pltpu.VMEM((8 * OUT, D), BF16),
                pltpu.SemaphoreType.DMA((2, 8)),
            ],
        ),
        out_shape=jax.ShapeDtypeStruct((2 * STEPS * SEQ, D), F32),
        input_output_aliases={19: 0} if chained else {},
        compiler_params=params(dimension_semantics=("arbitrary",)),
        cost_estimate=cost(2 * 2 * SEQ * D * D, 30e6),
    )(pos, y1, *os_, *ws, dep, *([chain] if chained else []))


def norm_back_kernel(steps, chained, base, *refs):
    n = len(steps)
    xs, fs, c2 = refs[: 2 * n], refs[2 * n : 10 * n], refs[10 * n]
    refs = refs[10 * n + (3 if chained else 2) :]
    out, f, sems = refs
    per = SEQ // ROWS
    i = pl.program_id(0)
    size = SEQ // 4

    def copies(k):
        return [
            pltpu.make_async_copy(fs[8 * k + j], f.at[k, pl.ds(pl.multiple_of(base[2 + j] * size, size), size), :], sems.at[k, j])
            for j in range(8)
        ]

    @pl.when(i == 0)
    def _():
        for k in range(n):
            for cp in copies(k):
                cp.start()

    for k in range(n):
        @pl.when(i == 2 * per * k)
        def _():
            for cp in copies(k):
                cp.wait()

    def run(k, seq, x_ref):
        owner = base[0] if seq == 0 else 1 - base[0]
        at0 = owner * SEQ + (i - (2 * k + seq) * per) * ROWS

        def rows(r, _):
            at = pl.ds(pl.multiple_of(r * 16, 16), 16)
            x = x_ref[at, :]
            q = inv_rms(x)
            nf = x * q
            g = f[k, pl.ds(pl.multiple_of(at0 + r * 16, 16), 16), :].astype(F32)
            out[at, :] = c2[at, :] + q * (g - nf * jnp.mean(nf * g, axis=-1, keepdims=True))
            return 0

        lax.fori_loop(0, ROWS // 16, rows, 0, unroll=4)

    for k in range(n):
        for seq in range(2):
            @pl.when(i // per == 2 * k + seq)
            def _():
                run(k, seq, xs[2 * k + seq])


def norm_back(steps, core, xs, fs, c2, dep, chain):
    per = SEQ // ROWS
    n = len(steps)
    chained = chain is not None

    def xspec(j):
        return pl.BlockSpec((ROWS, D), lambda i, base: (jnp.clip(i - j * per, 0, per - 1), 0))

    def at(i, base):
        owner = jnp.where((i // per) % 2 == 0, base[0], 1 - base[0])
        return (owner * (STEPS * per) + (steps[0] + i // (2 * per)) * per + i % per, 0)

    row = pl.BlockSpec((ROWS, D), at)
    return pl.pallas_call(
        functools.partial(norm_back_kernel, steps, chained),
        name="norm_back",
        grid_spec=pltpu.PrefetchScalarGridSpec(
            num_scalar_prefetch=1,
            grid=(2 * per * n,),
            in_specs=[xspec(j) for j in range(2 * n)] + [any_spec()] * (8 * n) + [row, any_spec()] + [any_spec()] * (1 if chained else 0),
            out_specs=row,
            scratch_shapes=[pltpu.VMEM((n, 2 * SEQ, D), BF16), pltpu.SemaphoreType.DMA((n, 8))],
        ),
        out_shape=jax.ShapeDtypeStruct((2 * STEPS * SEQ, D), F32),
        input_output_aliases={10 * n + 3: 0} if chained else {},
        compiler_params=params(dimension_semantics=("arbitrary",)),
        cost_estimate=cost(n * 4e9, n * 40e6),
    )(core, *xs, *fs, c2, dep, *([chain] if chained else []))


def solution(mesh):
    act_spec = P("dp", None, None)
    weight_specs = (P(None, None, "tp", None, None), P(None, "tp", None, None), P(None, None, "tp"), P(None, "tp", None))
    grad_specs = (P("dp", None, "tp", None, None), P("dp", "tp", None, None), P("dp", None, "tp"), P("dp", "tp", None))

    pairs = {
        "core": [(t, t ^ 1) for t in range(8)],
        "a": [(t, t ^ (4 if t & 1 else 2)) for t in range(8)],
        "b": [(t, t ^ (2 if t & 1 else 4)) for t in range(8)],
    }

    def swap(x, kind):
        return lax.ppermute(x, "tp", pairs[kind])

    def local_backward(out_y1, out_y2, cot_y1, cot_y2, w_qkv, w_out, w_up, w_down):
        rank = lax.axis_index("tp")
        core = rank & 1

        def near(r):
            return jnp.where(r & 1 == 0, (r >> 1) & 1, (r >> 2) & 1)

        def far(r):
            return jnp.where(r & 1 == 0, (r >> 2) & 1, (r >> 1) & 1)

        mask_a = jnp.where(core == 0, 2, 4)
        mask_b = jnp.where(core == 0, 4, 2)
        slots = [rank, rank ^ mask_a, rank ^ mask_b, rank ^ 6, rank ^ 1, rank ^ 1 ^ mask_b, rank ^ 1 ^ mask_a, rank ^ 7]
        pos = jnp.stack(slots).astype(jnp.int32)
        base = jnp.stack([core, near(rank)] + [(r & 1) * 4 + near(r) * 2 + far(r) for r in slots]).astype(jnp.int32)
        far_bit = far(rank)
        flat = lambda z: z.reshape(2 * STEPS * SEQ, D)
        y1, y2, c1, c2 = flat(out_y1), flat(out_y2), flat(cot_y1), flat(cot_y2)
        w1, w2 = w_up[0], w_down[0]
        wq = jnp.transpose(w_qkv[0], (1, 2, 3, 0)).reshape(QKV, D)
        wo = w_out[0].reshape(OUT, D)

        w1p, w2p = swap(w1, "core"), swap(w2, "core")
        w1a, w2a = swap(w1, "a"), swap(w2, "a")
        w1b, w2b = swap(w1, "b"), swap(w2, "b")
        n_all, cot_all, act, dh, gp, np_ = mlp_own(base, y1, c2, w1, w1p, w2, w2p)
        g1o, g1p = mlp_grad(False, n_all, dh, np_)
        w1a, w2a, w1b, w2b, wo, g1o = lax.optimization_barrier((w1a, w2a, w1b, w2b, wo, g1o))
        w1d, w2d = swap(w1b, "a"), swap(w2b, "a")
        rest_ab = [w1a, swap(w1a, "core"), w2a, swap(w2a, "core")]
        rest_ab += [w1b, swap(w1b, "core"), w2b, swap(w2b, "core")]
        g1r = swap(g1p, "core")
        g2o, g2p = mlp_grad(True, act, cot_all, g1o)
        g2r = swap(g2p, "core")
        common = (base, n_all, cot_all, y1, y2, c1, gp, np_)
        part = mlp_rest(0, *common, rest_ab, None, g2o, False)
        rest_d = [w1d, swap(w1d, "core"), w2d, swap(w2d, "core")]
        g_up = g1o + g1r
        g_down = g2o + g2r
        wos = [wo, swap(wo, "a"), swap(wo, "b")]
        wos.append(swap(wos[2], "a"))
        wos += [swap(w, "core") for w in wos]

        x2s, d1s = [None] * STEPS, [None] * STEPS
        ots, fns = [None] * STEPS, [None] * STEPS
        chain = x1 = dx2 = None
        fn_peer = oT_half = None

        def rest(s, dep):
            if s == 0:
                x, d = mlp_rest(0, *common, rest_d, part, dep, True)
            else:
                x, d = mlp_rest(s, *common, rest_ab + rest_d, None, dep, True)
            x2s[s], d1s[s] = (x, swap(x, "core")), (d, swap(d, "core"))
            return x

        def peer(s, dep):
            nonlocal chain, fn_peer, oT_half
            *chain, oT_half, fn = attn(s, True, base, x2s[s][1], d1s[s][1], wq, wo, None, None, dep, chain)
            fn_peer = swap(fn, "core")
            return fn

        def own(s, dep):
            nonlocal chain
            *chain, oT, go, stay = attn(s, False, base, x2s[s][0], d1s[s][0], wq, wo, fn_peer, oT_half, dep, chain)
            items = [oT, swap(oT, "a"), swap(oT, "b")]
            items.append(swap(items[2], "a"))
            ots[s] = items + [swap(o, "core") for o in items]
            got = swap(go, "a").reshape(2, SEQ // 4, D)
            stay = stay.reshape(2, SEQ // 4, D)
            pick = lambda z, k: lax.dynamic_index_in_dim(z, k, 0, keepdims=False)
            send = (pick(stay, 1 - far_bit) + pick(got, 1 - far_bit).astype(F32)).astype(BF16)
            got2 = swap(send, "b")
            quarter = (pick(stay, far_bit) + pick(got, far_bit).astype(F32) + got2.astype(F32)).astype(BF16)
            pieces = [quarter, swap(quarter, "a"), swap(quarter, "b")]
            pieces.append(swap(pieces[2], "a"))
            fns[s] = pieces + [swap(z, "core") for z in pieces]
            return go

        def proj(s, dep):
            nonlocal x1
            x1 = out_proj(s, pos, y1, ots[s], wos, y1 if dep is x1 else dep, x1)
            return x1

        def back(steps, dep):
            nonlocal dx2
            xs = [x for s in steps for x in x2s[s]]
            fs = [f for s in steps for f in fns[s]]
            dx2 = norm_back(steps, base, xs, fs, c2, c2 if dep is dx2 else dep, dx2)
            return dx2

        t = rest(0, part[0])
        for call in (
            (rest, 1), (peer, 0), (rest, 2), (own, 0), (peer, 1), (rest, 3), (own, 1), (peer, 2), (proj, 0), (own, 2),
            (peer, 3), (proj, 1), (own, 3), (back, (0, 1)), (proj, 2), (proj, 3), (back, (2,)), (back, (3,)),
        ):
            t = call[0](call[1], t)

        x2, dx1, aq, ao = chain
        full = lambda z: z.reshape(2 * STEPS, SEQ, D)
        g_qkv = jnp.transpose(aq.reshape(HEADS_DEV, 3, HEAD, D), (3, 0, 1, 2))
        g_out = ao.reshape(HEADS_DEV, HEAD, D)
        return full(x1), full(x2), full(dx1), full(dx2), g_qkv[None], g_out[None], g_up[None], g_down[None]

    return jax.shard_map(
        local_backward,
        mesh=mesh,
        in_specs=(act_spec,) * 4 + weight_specs,
        out_specs=(act_spec,) * 4 + grad_specs,
        check_vma=False,
    )
```
